32 devices in a mesh: rep: 1 (over z), mp: 4 (over y), tb: 4 (over x), ta: 2 (over core).
Axes of the slice: x: 4, y: 4, z: 1, core: 2. Of those that a mesh axis runs over, the one named last changes fastest.
The devices are a block of a 4x4x8 slice.
Arguments:
- x_in: bfloat16 [16384, 2048], P(('rep', 'tb', 'ta'), 'mp')
- seg_ids: int32 [16384], P(('rep', 'tb', 'ta'))
- pos_ids: int32 [16384], P(('rep', 'tb', 'ta'))
- w_q: bfloat16 [2, 2048, 2048], P(None, ('tb', 'ta'), 'mp')
- w_k: bfloat16 [2, 2048, 128], P(None, ('tb', 'ta'))
- w_v: bfloat16 [2, 2048, 128], P(None, ('tb', 'ta'))
- w_gate: bfloat16 [2, 2048, 8192], P(None, ('tb', 'ta'), 'mp')
- w_up: bfloat16 [2, 2048, 8192], P(None, ('tb', 'ta'), 'mp')
- w_out: bfloat16 [2, 2048, 2048], P(None, 'mp', ('tb', 'ta'))
- w_down: bfloat16 [2, 8192, 2048], P(None, 'mp', ('tb', 'ta'))
- norm_gain: bfloat16 [2, 2048], replicated
Outputs:
- output: float32 [16384, 2048], P(('rep', 'tb', 'ta'), 'mp')
All inputs are finite; a program needn't handle non-finite values.
Results may differ from the reference program's by a relative error of at most 0.00516327.
Values are sent between devices in bfloat16 or wider.
A program may use at most 768 MiB of HBM per device.

```python
import jax
import jax.numpy as jnp
from jax import lax

TOKENS = 16384
BLOCK_TOKENS = 2048
EMBED = 2048
HEADS = 16
HEAD_DIM = 128
FFN_DIM = 8192
LAYERS = 2
NUM_BLOCKS = TOKENS // BLOCK_TOKENS
REQ_MEAN = max(2, min(BLOCK_TOKENS // 2, 64))
ROPE_BASE = 10000.0
NORM_EPS = 1e-6


def draw_requests(key):
    starts = jax.random.randint(key, (NUM_BLOCKS, BLOCK_TOKENS), 0, REQ_MEAN) == 0
    block_start = (jnp.arange(BLOCK_TOKENS) == 0)[None, :]
    start_flags = (starts | block_start).reshape(TOKENS).astype(jnp.int32)
    tok_index = jnp.arange(TOKENS, dtype=jnp.int32)
    seg_ids = jnp.cumsum(start_flags).astype(jnp.int32) - 1
    pos_ids = tok_index - lax.cummax(start_flags * tok_index, axis=0)
    return seg_ids, pos_ids


def normal_weight(key, shape, fan_in, scale_mult):
    return (jax.random.normal(key, shape, jnp.float32) * (scale_mult * fan_in ** -0.5)).astype(jnp.bfloat16)


def setup_inputs(seed: int = 0, part: int = 0) -> dict:
    part_key = jax.random.fold_in(jax.random.key(seed), part)
    key_x, key_req = jax.random.split(part_key)
    shared = jax.random.split(jax.random.key(seed + 1), 8)
    seg_ids, pos_ids = draw_requests(key_req)
    width_q = HEADS * HEAD_DIM
    return {
        "x_in": jax.random.normal(key_x, (TOKENS, EMBED), jnp.float32).astype(jnp.bfloat16),
        "seg_ids": seg_ids,
        "pos_ids": pos_ids,
        "w_q": normal_weight(shared[0], (LAYERS, EMBED, width_q), EMBED, 1.0),
        "w_k": normal_weight(shared[1], (LAYERS, EMBED, HEAD_DIM), EMBED, 1.0),
        "w_v": normal_weight(shared[2], (LAYERS, EMBED, HEAD_DIM), EMBED, 1.0),
        "w_gate": normal_weight(shared[3], (LAYERS, EMBED, FFN_DIM), EMBED, 1.0),
        "w_up": normal_weight(shared[4], (LAYERS, EMBED, FFN_DIM), EMBED, 1.0),
        "w_out": normal_weight(shared[5], (LAYERS, width_q, EMBED), width_q, 2.0),
        "w_down": normal_weight(shared[6], (LAYERS, FFN_DIM, EMBED), FFN_DIM, 1.0),
        "norm_gain": jax.random.uniform(shared[7], (LAYERS, EMBED), jnp.float32, 0.5, 1.5).astype(jnp.bfloat16),
    }


def apply_rope(rot_in, cos_tab, sin_tab):
    half_dim = HEAD_DIM // 2
    lower_half = rot_in[..., :half_dim].astype(jnp.float32)
    upper_half = rot_in[..., half_dim:].astype(jnp.float32)
    return jnp.concatenate([lower_half * cos_tab - upper_half * sin_tab, upper_half * cos_tab + lower_half * sin_tab], axis=-1).astype(jnp.bfloat16)


def layer_block(hidden, seg_blk, pos_blk, w_q, w_k, w_v, w_gate, w_up, w_out, w_down, gain):
    mean_sq = jnp.mean(hidden * hidden, axis=-1, keepdims=True)
    normed = (hidden * lax.rsqrt(mean_sq + NORM_EPS) * gain.astype(jnp.float32)).astype(jnp.bfloat16)
    q_proj = jnp.dot(normed, w_q, preferred_element_type=jnp.float32).astype(jnp.bfloat16)
    k_proj = jnp.dot(normed, w_k, preferred_element_type=jnp.float32).astype(jnp.bfloat16)
    v_proj = jnp.dot(normed, w_v, preferred_element_type=jnp.float32).astype(jnp.bfloat16)
    gate_proj = jnp.dot(normed, w_gate, preferred_element_type=jnp.float32).astype(jnp.bfloat16)
    up_proj = jnp.dot(normed, w_up, preferred_element_type=jnp.float32).astype(jnp.bfloat16)
    half_dim = HEAD_DIM // 2
    inv_freq = ROPE_BASE ** (-(jnp.arange(half_dim, dtype=jnp.float32) * 2.0) / HEAD_DIM)
    angles = pos_blk.astype(jnp.float32)[:, None] * inv_freq[None, :]
    cos_tab = jnp.cos(angles)
    sin_tab = jnp.sin(angles)
    q_rot = apply_rope(q_proj.reshape(BLOCK_TOKENS, HEADS, HEAD_DIM), cos_tab[:, None, :], sin_tab[:, None, :])
    k_rot = apply_rope(k_proj, cos_tab, sin_tab)
    allowed = (seg_blk[:, None] == seg_blk[None, :]) & (pos_blk[None, :] <= pos_blk[:, None])
    score_scale = HEAD_DIM ** -0.5

    def one_head(q_head):
        scores = jnp.dot(q_head, k_rot.T, preferred_element_type=jnp.float32) * score_scale
        scores = jnp.where(allowed, scores, -1e30)
        row_peak = jnp.max(scores, axis=-1, keepdims=True)
        exp_scores = jnp.exp(scores - row_peak)
        prob_bf16 = (exp_scores / jnp.sum(exp_scores, axis=-1, keepdims=True)).astype(jnp.bfloat16)
        return jnp.dot(prob_bf16, v_proj, preferred_element_type=jnp.float32).astype(jnp.bfloat16)

    attn_heads = lax.map(one_head, jnp.transpose(q_rot, (1, 0, 2)))
    attn = jnp.transpose(attn_heads, (1, 0, 2)).reshape(BLOCK_TOKENS, HEADS * HEAD_DIM)
    mlp_act = (jax.nn.silu(gate_proj.astype(jnp.float32)) * up_proj.astype(jnp.float32)).astype(jnp.bfloat16)
    branch = jnp.dot(attn, w_out, preferred_element_type=jnp.float32) + jnp.dot(mlp_act, w_down, preferred_element_type=jnp.float32)
    return hidden + branch


def reference(x_in, seg_ids, pos_ids, w_q, w_k, w_v, w_gate, w_up, w_out, w_down, norm_gain):
    seg_blocks = seg_ids.reshape(NUM_BLOCKS, BLOCK_TOKENS)
    pos_blocks = pos_ids.reshape(NUM_BLOCKS, BLOCK_TOKENS)

    def layer_step(hidden, weights):
        def block_step(blk):
            return layer_block(blk[0], blk[1], blk[2], weights[0], weights[1], weights[2], weights[3], weights[4], weights[5], weights[6], weights[7])

        hidden_blocks = lax.map(block_step, (hidden.reshape(NUM_BLOCKS, BLOCK_TOKENS, EMBED), seg_blocks, pos_blocks))
        return hidden_blocks.reshape(TOKENS, EMBED), None

    final_x, unused = lax.scan(layer_step, x_in.astype(jnp.float32), (w_q, w_k, w_v, w_gate, w_up, w_out, w_down, norm_gain))
    return final_x
```

```python
import functools

import jax
import jax.numpy as jnp
from jax import lax
from jax.experimental import pallas as pl
from jax.experimental.pallas import tpu as pltpu
from jax.sharding import PartitionSpec as P


ROPE_BASE = 10000.0
NORM_EPS = 1e-6
TOKEN_AXES = ("rep", "tb", "ta")
PLANE_AXES = ("tb", "ta")
F32 = jnp.float32
BF16 = jnp.bfloat16
ROWS = 512
Q_TILE = 128
K_TILE = 256
VMEM_LIMIT = 60 * 1024 * 1024


def dot(a, b):
    return jnp.dot(a, b, preferred_element_type=F32)


def rope(t, cos_tab, sin_tab):
    half = t.shape[-1] // 2
    t = t.astype(F32)
    swapped = jnp.concatenate([t[:, half:], t[:, :half]], axis=1)
    return (t * cos_tab + swapped * sin_tab).astype(BF16)


def in_proj_kernel(stacked, blocks, head_dim, blk_ref, x_ref, gain_ref, cos_ref, sin_ref, *refs):
    a_refs, b_refs = refs[:blocks], refs[blocks : 2 * blocks]
    q_ref, k_ref, v_ref, m_ref, h_ref = refs[2 * blocks :]
    step = pl.program_id(0)
    depth = a_refs[0].shape[0]
    tokens = h_ref.shape[0]

    def product(rows, w_refs, width):
        total = None
        for p, w in enumerate(w_refs):
            term = dot(h_ref[rows, p * depth : (p + 1) * depth], w[:, :width])
            total = term if total is None else total + term
        return total.astype(BF16)

    def first(i, carry):
        rows = pl.ds(pl.multiple_of(i * ROWS, ROWS), ROWS)
        if stacked:
            parts, _, span = x_ref.shape
            total = jnp.zeros((ROWS, 1), F32)
            for r in range(parts):
                xs = x_ref[r, rows, :].astype(F32)
                total += jnp.sum(xs * xs, axis=1, keepdims=True)
            inv = lax.rsqrt(total / (parts * span) + NORM_EPS)
            per = span // depth
            for p in range(blocks):
                blk = blk_ref[p]
                part = blk // per
                col = pl.ds(pl.multiple_of((blk % per) * depth, depth), depth)
                xs = x_ref[part, rows, col].astype(F32)
                h_ref[rows, p * depth : (p + 1) * depth] = (xs * inv * gain_ref[part, :, col].astype(F32)).astype(BF16)
        else:
            for p in range(blocks):
                col = pl.ds(pl.multiple_of(blk_ref[p] * depth, depth), depth)
                h_ref[rows, p * depth : (p + 1) * depth] = x_ref[rows, col]
        q = product(rows, a_refs, q_ref.shape[1])
        cos_tab, sin_tab = cos_ref[rows, :], sin_ref[rows, :]
        for n in range(q_ref.shape[1] // head_dim):
            cols = slice(n * head_dim, (n + 1) * head_dim)
            q_ref[rows, cols] = rope(q[:, cols], cos_tab, sin_tab)
        kv = product(rows, b_refs, 2 * head_dim)
        k_ref[rows, :] = rope(kv[:, :head_dim], cos_tab, sin_tab)
        v_ref[rows, :] = kv[:, head_dim:]
        return carry

    def later(i, carry):
        rows = pl.ds(pl.multiple_of(i * ROWS, ROWS), ROWS)
        width = m_ref.shape[1]
        gate = product(rows, a_refs, width).astype(F32)
        up = product(rows, b_refs, width).astype(F32)
        m_ref[rows, :] = (gate * (1.0 / (1.0 + jnp.exp(-gate))) * up).astype(BF16)
        return carry

    @pl.when(step == 0)
    def _():
        lax.fori_loop(0, tokens // ROWS, first, 0)

    @pl.when(step > 0)
    def _():
        lax.fori_loop(0, tokens // ROWS, later, 0)


def in_proj(x, gain, cos_tab, sin_tab, blk, a_pieces, b_pieces, width_q, width_ff, head_dim, stacked):
    blocks = len(a_pieces)
    depth = a_pieces[0].shape[0]
    embed = blocks * depth
    tile = width_q
    tiles = width_ff // tile
    tokens = cos_tab.shape[0]
    whole = lambda a: pl.BlockSpec(a.shape, lambda i, s: (0,) * a.ndim, pipeline_mode=pl.Buffered(1))
    a_spec = pl.BlockSpec((depth, tile), lambda i, s: (0, i))
    b_spec = pl.BlockSpec((depth, tile), lambda i, s: (0, jnp.where(i == 0, tiles, i - 1)))
    return pl.pallas_call(
        functools.partial(in_proj_kernel, stacked, blocks, head_dim),
        grid_spec=pltpu.PrefetchScalarGridSpec(
            num_scalar_prefetch=1,
            grid=(tiles + 1,),
            in_specs=[whole(x), whole(gain), whole(cos_tab), whole(sin_tab)] + [a_spec] * blocks + [b_spec] * blocks,
            out_specs=[
                pl.BlockSpec((tokens, width_q), lambda i, s: (0, 0)),
                pl.BlockSpec((tokens, head_dim), lambda i, s: (0, 0)),
                pl.BlockSpec((tokens, head_dim), lambda i, s: (0, 0)),
                pl.BlockSpec((tokens, tile), lambda i, s: (0, jnp.maximum(i - 1, 0))),
            ],
            scratch_shapes=[pltpu.VMEM((tokens, embed), BF16)],
        ),
        out_shape=[
            jax.ShapeDtypeStruct((tokens, width_q), BF16),
            jax.ShapeDtypeStruct((tokens, head_dim), BF16),
            jax.ShapeDtypeStruct((tokens, head_dim), BF16),
            jax.ShapeDtypeStruct((tokens, width_ff), BF16),
        ],
        compiler_params=pltpu.CompilerParams(vmem_limit_bytes=VMEM_LIMIT),
        cost_estimate=pl.CostEstimate(
            flops=2 * tokens * embed * (width_q + 2 * head_dim + 2 * width_ff),
            bytes_accessed=2 * embed * (width_q + 2 * head_dim + 2 * width_ff),
            transcendentals=tokens * width_ff,
        ),
        name="in_proj",
    )(blk, x, gain, cos_tab, sin_tab, *a_pieces, *b_pieces)


def attention_kernel(base, head_dim, low_ref, start_ref, q_ref, k_ref, v_ref, o_ref, s_ref):
    tile = pl.program_id(0)
    rows = q_ref.shape[0]
    heads = q_ref.shape[1] // head_dim
    first = base + tile * rows
    q = jnp.concatenate([q_ref[:, i * head_dim : (i + 1) * head_dim] for i in range(heads)], axis=0)
    low = low_ref[base // rows + tile] // K_TILE
    high = (first + rows + K_TILE - 1) // K_TILE
    start = start_ref[...]
    own = first + lax.broadcasted_iota(jnp.int32, (rows, 1), 0)
    scale = head_dim**-0.5

    def score(t, peak):
        keys = pl.ds(pl.multiple_of(t * K_TILE, K_TILE), K_TILE)
        s = lax.dot_general(q, k_ref[keys, :], (((1,), (1,)), ((), ())), preferred_element_type=F32) * scale
        key = t * K_TILE + lax.broadcasted_iota(jnp.int32, (rows, K_TILE), 1)
        allowed = (key >= start) & (key <= own)
        s = jnp.where(jnp.concatenate([allowed] * heads, axis=0), s, -1e30)
        s_ref[t] = s
        return jnp.maximum(peak, jnp.max(s, axis=1, keepdims=True))

    peak = lax.fori_loop(low, high, score, jnp.full((heads * rows, 1), -1e30, F32))

    def expo(t, total):
        e = jnp.exp(s_ref[t] - peak)
        s_ref[t] = e
        return total + jnp.sum(e, axis=1, keepdims=True)

    total = lax.fori_loop(low, high, expo, jnp.zeros((heads * rows, 1), F32))
    inv = 1.0 / total

    def value(t, acc):
        keys = pl.ds(pl.multiple_of(t * K_TILE, K_TILE), K_TILE)
        return acc + dot((s_ref[t] * inv).astype(BF16), v_ref[keys, :])

    out = lax.fori_loop(low, high, value, jnp.zeros((heads * rows, head_dim), F32)).astype(BF16)
    for i in range(heads):
        o_ref[:, i * head_dim : (i + 1) * head_dim] = out[i * rows : (i + 1) * rows]


def attention(q, k, v, low, start):
    rows, width_q = q.shape
    keys, head_dim = k.shape
    base = 0
    tiles = rows // Q_TILE
    return pl.pallas_call(
        functools.partial(attention_kernel, base, head_dim),
        grid_spec=pltpu.PrefetchScalarGridSpec(
            num_scalar_prefetch=1,
            grid=(tiles,),
            in_specs=[
                pl.BlockSpec((Q_TILE, 1), lambda i, s: (base // Q_TILE + i, 0)),
                pl.BlockSpec((Q_TILE, width_q), lambda i, s: (i, 0)),
                pl.BlockSpec((keys, head_dim), lambda i, s: (0, 0)),
                pl.BlockSpec((keys, head_dim), lambda i, s: (0, 0)),
            ],
            out_specs=pl.BlockSpec((Q_TILE, width_q), lambda i, s: (i, 0)),
            scratch_shapes=[pltpu.VMEM((keys // K_TILE, width_q // head_dim * Q_TILE, K_TILE), F32)],
        ),
        out_shape=jax.ShapeDtypeStruct((rows, width_q), BF16),
        compiler_params=pltpu.CompilerParams(vmem_limit_bytes=VMEM_LIMIT),
        cost_estimate=pl.CostEstimate(flops=8 * rows * width_q * 512, bytes_accessed=4 * rows * width_q, transcendentals=rows * 2048),
        name="attention",
    )(low, start, q, k, v)


def back_kernel(blocks, parts, last, sizes, o_ref, m_ref, res_ref, *refs):
    pieces = refs[: blocks + 2]
    out_ref, w_ref, sent_ref, got_ref, w_sem, send_sem, recv_sem = refs[blocks + 2 :]
    tb_size, ta_size = sizes
    me, tb, ta = lax.axis_index("mp"), lax.axis_index("tb"), lax.axis_index("ta")
    streams, hops = got_ref.shape[0], got_ref.shape[1]
    width_q = o_ref.shape[1]
    cols = w_ref.shape[2]
    high, wide = got_ref.shape[2], got_ref.shape[3]

    loads = []
    for p in range(blocks):
        off = (0, tb_size - 1, 1, 2)[p // 2]
        at = lax.rem(tb + off, tb_size) * ta_size + lax.rem(ta + p % 2, ta_size)
        if p < blocks - 2:
            loads.append(pltpu.make_async_copy(pieces[p], w_ref.at[at], w_sem.at[p]))
        else:
            for n in range(2):
                i = blocks - 2 + 2 * (p - blocks + 2) + n
                half = pieces[i].shape[0]
                loads.append(pltpu.make_async_copy(pieces[i], w_ref.at[at, pl.ds(n * half, half)], w_sem.at[i]))
    for load in loads:
        load.start()

    barrier = pltpu.get_barrier_semaphore()
    for near in (1, parts - 1):
        pl.semaphore_signal(barrier, inc=1, device_id={"mp": lax.rem(me + near, parts)}, device_id_type=pl.DeviceIdType.MESH)
    for load in loads:
        load.wait()
    pl.semaphore_wait(barrier, 2)

    def partial(stream, dest):
        if last:
            rows = pl.ds(pl.multiple_of(stream * high, high), high)
            first = dest * (wide // cols)
            tiles = [first + n for n in range(wide // cols)]
        else:
            rows = pl.ds(pl.multiple_of(dest * high, high), high)
            tiles = [stream]
        o, m = o_ref[rows, :], m_ref[rows, :]
        sums = [dot(o, w_ref[t, :width_q, :]) + dot(m, w_ref[t, width_q:, :]) for t in tiles]
        return sums[0] if len(sums) == 1 else jnp.concatenate(sums, axis=1)

    def hop(stream, step):
        up = stream < streams // 2
        return pltpu.make_async_remote_copy(
            src_ref=sent_ref.at[stream] if step == 0 else got_ref.at[stream, step - 1],
            dst_ref=got_ref.at[stream, step],
            send_sem=send_sem.at[stream, step],
            recv_sem=recv_sem.at[stream, step],
            device_id={"mp": lax.rem(me + jnp.where(up, 1, parts - 1), parts)},
            device_id_type=pl.DeviceIdType.MESH,
        )

    for step in range(hops + 1):

        def body(i, carry):
            stream = lax.rem(i, 2) * (streams // 2) + i // 2
            up = stream < streams // 2
            dest = lax.rem(me + jnp.where(up, 2 * parts - 1 - step, 1 + step), parts)
            value = partial(stream, dest)
            if last:
                held = res_ref.shape[0]
                per = held // high

                def with_residual(v):
                    here = pl.ds(pl.multiple_of(lax.rem(stream, per) * high, high), high)
                    there = pl.ds(pl.multiple_of(dest * wide, wide), wide)
                    mine = jnp.where(stream // per == me, 1.0, 0.0)
                    return v + res_ref[here, there] * mine

                value = with_residual(value)
            if step > 0:
                hop(stream, step - 1).wait_recv()
                value += got_ref[stream, step - 1]
            if step == 0:
                sent_ref[stream] = value
            elif step < hops:
                got_ref[stream, step - 1] = value
            if step < hops:
                hop(stream, step).start()
            elif last:
                out_ref[pl.ds(pl.multiple_of(stream * high, high), high), :] = value
            else:
                per = res_ref.shape[2] // cols
                col = pl.ds(pl.multiple_of(lax.rem(stream, per) * cols, cols), cols)
                out_ref[:, pl.ds(pl.multiple_of(stream * cols, cols), cols)] = value + res_ref[stream // per, :, col].astype(F32)
            return carry

        lax.fori_loop(0, streams, body, 0)

    for step in range(hops):

        def drain(stream, carry):
            hop(stream, step).wait_send()
            return carry

        lax.fori_loop(0, streams, drain, 0)


def back(o, m, res, pieces, parts, sizes, last, collective_id):
    tokens, _ = o.shape
    blocks = len(pieces) - 2
    depth, cols = pieces[0].shape
    embed = blocks * cols
    streams, hops = blocks, parts - 1
    if last:
        shape, out = (tokens // streams, embed // parts), (tokens, embed // parts)
    else:
        shape, out = (tokens // parts, cols), (tokens // parts, embed)
    vmem = pl.BlockSpec(memory_space=pltpu.VMEM)
    return pl.pallas_call(
        functools.partial(back_kernel, blocks, parts, last, sizes),
        in_specs=[vmem, vmem, vmem] + [pl.BlockSpec(memory_space=pl.ANY)] * len(pieces),
        out_specs=vmem,
        out_shape=jax.ShapeDtypeStruct(out, F32),
        scratch_shapes=[
            pltpu.VMEM((blocks, depth, cols), BF16),
            pltpu.VMEM((streams, *shape), F32),
            pltpu.VMEM((streams, hops, *shape), F32),
            pltpu.SemaphoreType.DMA((len(pieces),)),
            pltpu.SemaphoreType.DMA((streams, hops)),
            pltpu.SemaphoreType.DMA((streams, hops)),
        ],
        compiler_params=pltpu.CompilerParams(vmem_limit_bytes=VMEM_LIMIT, collective_id=collective_id, has_side_effects=True),
        cost_estimate=pl.CostEstimate(flops=8 * tokens * depth * embed, bytes_accessed=2 * depth * embed, transcendentals=0),
        name="back",
    )(o, m, res, *pieces)


def solution(mesh):
    mp_size, tb_size, ta_size = mesh.shape["mp"], mesh.shape["tb"], mesh.shape["ta"]
    assert tb_size == 4 and ta_size == 2
    right = [(i, (i + 1) % tb_size) for i in range(tb_size)]
    left = [(i, (i - 1) % tb_size) for i in range(tb_size)]
    swap = [(0, 1), (1, 0)]

    def after(values, *deps):
        return lax.optimization_barrier((*values, *deps))[: len(values)]

    def both(piece):
        return piece, lax.ppermute(piece, "ta", swap)

    def body(x_loc, seg_ids, pos_ids, w_q, w_k, w_v, w_gate, w_up, w_out, w_down, gain):
        tokens, embed_loc = x_loc.shape
        head_dim, width_q, width_ff = w_k.shape[-1], w_q.shape[-1], w_gate.shape[-1]
        layers = w_q.shape[0]
        tb, ta, mp = lax.axis_index("tb"), lax.axis_index("ta"), lax.axis_index("mp")
        offsets = jnp.array([0, 0, -1, -1, 1, 1, 2, 2], jnp.int32)
        other = jnp.array([0, 1] * 4, jnp.int32)
        blk = lax.rem(tb + offsets + tb_size, tb_size) * ta_size + lax.rem(ta + other, ta_size)

        inv_freq = ROPE_BASE ** (-(jnp.arange(head_dim // 2, dtype=F32) * 2.0) / head_dim)
        angles = pos_ids.astype(F32)[:, None] * inv_freq[None, :]
        cos_tab, sin_tab = jnp.cos(angles), jnp.sin(angles)
        cos_tab = jnp.concatenate([cos_tab, cos_tab], axis=1)
        sin_tab = jnp.concatenate([-sin_tab, sin_tab], axis=1)
        start = jnp.arange(tokens, dtype=jnp.int32) - pos_ids
        low = start[::Q_TILE]
        start = start[:, None]

        x_all = lax.all_gather(x_loc, "mp", axis=0, tiled=False)
        share = tokens // mp_size
        inputs = x_all
        residual = lax.dynamic_slice_in_dim(x_all, mp * share, share, axis=1)
        links_free = None
        for l in range(layers):
            last = l == layers - 1
            a = jnp.concatenate([w_q[l], w_gate[l]], axis=1)
            b = jnp.concatenate([w_up[l], w_k[l], w_v[l]], axis=1)
            c = jnp.concatenate([w_out[l], w_down[l]], axis=0)
            if l:
                a, b = after((a, b), *links_free)
            a_l, b_l = lax.ppermute(a, "tb", right), lax.ppermute(b, "tb", right)
            a_r, b_r = lax.ppermute(a, "tb", left), lax.ppermute(b, "tb", left)
            if l:
                a_l, b_l, a_r, b_r = after((a_l, b_l, a_r, b_r), inputs_ready)
            a_o, b_o = lax.ppermute(a_l, "tb", right), lax.ppermute(b_r, "tb", left)
            a_all = sum((both(t) for t in (a, a_l, a_r, a_o)), ())
            b_all = sum((both(t) for t in (b, b_l, b_r, b_o)), ())
            (c,) = after((c,), a_l, b_l, a_r, b_r)
            c_l, c_r = lax.ppermute(c, "tb", right), lax.ppermute(c, "tb", left)

            gain_l = gain[l].reshape(mp_size, 1, embed_loc)
            q, k, v, m = in_proj(inputs, gain_l, cos_tab, sin_tab, blk, a_all, b_all, width_q, width_ff, head_dim, l == 0)

            c_l, c_r = after((c_l, c_r), k)
            half = c.shape[0] // 2
            top = lax.ppermute(c_l[:half], "tb", right)
            low_half = lax.ppermute(c_r[half:], "tb", left)
            c_all = sum((both(t) for t in (c, c_l, c_r)), ())

            o = attention(q, k, v, low, start)

            top, low_half = after((top, low_half), o)
            top, low_half = both(top), both(low_half)
            c_all = c_all + (top[0], low_half[0], top[1], low_half[1])
            links_free = (top[0], low_half[0])
            hidden = back(o, m, residual, c_all, mp_size, (tb_size, ta_size), last, 1 + l)
            if last:
                return hidden
            residual = inputs_ready = hidden
            inv = lax.rsqrt(jnp.mean(hidden * hidden, axis=-1, keepdims=True) + NORM_EPS)
            h = (hidden * inv * gain[l + 1].astype(F32)).astype(BF16)
            inputs = lax.all_gather(h, "mp", axis=0, tiled=True)

    col_spec = P(None, PLANE_AXES, "mp")
    kv_spec = P(None, PLANE_AXES, None)
    row_spec = P(None, "mp", PLANE_AXES)
    return jax.shard_map(
        body,
        mesh=mesh,
        in_specs=(P(TOKEN_AXES, "mp"), P(TOKEN_AXES), P(TOKEN_AXES), col_spec, kv_spec, kv_spec, col_spec, col_spec, row_spec, row_spec, P(None, None)),
        out_specs=P(TOKEN_AXES, "mp"),
        check_vma=False,
    )
```

```python
import functools

import jax
import jax.numpy as jnp
from jax import lax
from jax.experimental import pallas as pl
from jax.experimental.pallas import tpu as pltpu
from jax.sharding import PartitionSpec as P

ROPE_BASE = 10000.0
NORM_EPS = 1e-6
TOKEN_AXES = ("rep", "tb", "ta")
PLANE_AXES = ("tb", "ta")
F32 = jnp.float32
BF16 = jnp.bfloat16
ROWS = 512
Q_TILE = 128
K_TILE = 256
NEAR = 256
VMEM_LIMIT = 60 * 1024 * 1024


def dot(a, b):
    return jnp.dot(a, b, preferred_element_type=F32)


def rope(t, cos_tab, sin_tab):
    half = t.shape[-1] // 2
    t = t.astype(F32)
    swapped = jnp.concatenate([t[:, half:], t[:, :half]], axis=1)
    return (t * cos_tab + swapped * sin_tab).astype(BF16)


def attention_kernel(head_dim, low_ref, start_ref, q_ref, k_ref, v_ref, o_ref, s_ref, acc_ref):
    tile = pl.program_id(0)
    rows = q_ref.shape[0]
    heads = q_ref.shape[1] // head_dim
    first = tile * rows
    q = jnp.concatenate([q_ref[:, i * head_dim : (i + 1) * head_dim] for i in range(heads)], axis=0)
    begin = low_ref[tile]
    base = jnp.maximum(first - NEAR, 0)
    low = begin // K_TILE
    high = (first + rows + K_TILE - 1) // K_TILE
    start = start_ref[...]
    own = first + lax.broadcasted_iota(jnp.int32, (1, rows), 1)
    scale = head_dim**-0.5

    @pl.when(begin >= base)
    def _():
        span = NEAR + rows
        keys = pl.ds(pl.multiple_of(base, 128), span)
        s = lax.dot_general(k_ref[keys, :], q, (((1,), (1,)), ((), ())), preferred_element_type=F32) * scale
        key = base + lax.broadcasted_iota(jnp.int32, (span, rows), 0)
        allowed = (key >= start) & (key <= own)
        for i in range(heads):
            t = jnp.where(allowed, s[:, i * rows : (i + 1) * rows], -1e30)
            e = jnp.exp(t - jnp.max(t, axis=0, keepdims=True))
            p = (e * (1.0 / jnp.sum(e, axis=0, keepdims=True))).astype(BF16)
            acc_ref[:, i * rows : (i + 1) * rows] = lax.dot_general(v_ref[keys, :], p, (((0,), (0,)), ((), ())), preferred_element_type=F32)

    @pl.when(begin < base)
    def _():
        def score(t, peak):
            keys = pl.ds(pl.multiple_of(t * K_TILE, K_TILE), K_TILE)
            s = lax.dot_general(k_ref[keys, :], q, (((1,), (1,)), ((), ())), preferred_element_type=F32) * scale
            key = t * K_TILE + lax.broadcasted_iota(jnp.int32, (K_TILE, rows), 0)
            allowed = (key >= start) & (key <= own)
            s = jnp.concatenate([jnp.where(allowed, s[:, i * rows : (i + 1) * rows], -1e30) for i in range(heads)], axis=1)
            s_ref[t] = s
            return jnp.maximum(peak, jnp.max(s, axis=0, keepdims=True))

        peak = lax.fori_loop(low, high, score, jnp.full((1, heads * rows), -1e30, F32))

        def expo(t, total):
            e = jnp.exp(s_ref[t] - peak)
            s_ref[t] = e
            return total + jnp.sum(e, axis=0, keepdims=True)

        total = lax.fori_loop(low, high, expo, jnp.zeros((1, heads * rows), F32))
        inv = 1.0 / total
        acc_ref[...] = jnp.zeros_like(acc_ref)

        def value(t, carry):
            keys = pl.ds(pl.multiple_of(t * K_TILE, K_TILE), K_TILE)
            p = (s_ref[t] * inv).astype(BF16)
            acc_ref[...] += lax.dot_general(v_ref[keys, :], p, (((0,), (0,)), ((), ())), preferred_element_type=F32)
            return carry

        lax.fori_loop(low, high, value, 0)

    for i in range(heads):
        o_ref[:, i * head_dim : (i + 1) * head_dim] = acc_ref[:, i * rows : (i + 1) * rows].T.astype(BF16)


def attention(q, k, v, low, start):
    rows, width_q = q.shape
    keys, head_dim = k.shape
    stacked = width_q // head_dim * Q_TILE
    return pl.pallas_call(
        functools.partial(attention_kernel, head_dim),
        grid_spec=pltpu.PrefetchScalarGridSpec(
            num_scalar_prefetch=1,
            grid=(rows // Q_TILE,),
            in_specs=[
                pl.BlockSpec((1, Q_TILE), lambda i, s: (0, i)),
                pl.BlockSpec((Q_TILE, width_q), lambda i, s: (i, 0)),
                pl.BlockSpec((keys, head_dim), lambda i, s: (0, 0)),
                pl.BlockSpec((keys, head_dim), lambda i, s: (0, 0)),
            ],
            out_specs=pl.BlockSpec((Q_TILE, width_q), lambda i, s: (i, 0)),
            scratch_shapes=[pltpu.VMEM((keys // K_TILE, K_TILE, stacked), F32), pltpu.VMEM((head_dim, stacked), F32)],
        ),
        out_shape=jax.ShapeDtypeStruct((rows, width_q), BF16),
        compiler_params=pltpu.CompilerParams(vmem_limit_bytes=VMEM_LIMIT),
        cost_estimate=pl.CostEstimate(flops=8 * rows * width_q * 512, bytes_accessed=4 * rows * width_q, transcendentals=rows * 2048),
        name="attention",
    )(low, start, q, k, v)


def place(p, tb, ta, tb_size, ta_size):
    return lax.rem(tb + (0, tb_size - 1, 1, 2)[p // 2], tb_size) * ta_size + lax.rem(ta + p % 2, ta_size)


def first_kernel(parts, head_dim, sizes, x_own, gain_ref, cos_ref, sin_ref, a0, b0, a1, b1, c, q_ref, k_ref, v_ref, m_ref, res_ref, c_got, x_ref, h_ref, wa0, wb0, wa1, wb1, own_sem, send_sem, recv_sem):
    tb_size, ta_size = sizes
    me, tb, ta = lax.axis_index("mp"), lax.axis_index("tb"), lax.axis_index("ta")
    y_up, y_down = lax.rem(me + 1, parts), lax.rem(me + parts - 1, parts)
    x_up, x_down = {"tb": lax.rem(tb + 1, tb_size)}, {"tb": lax.rem(tb + tb_size - 1, tb_size)}
    core = {"ta": lax.rem(ta + 1, ta_size)}
    tokens, span = x_own.shape
    depth = a0.shape[0]
    width_q, width_ff = q_ref.shape[1], m_ref.shape[1]
    part_ff = width_ff // 2
    share = res_ref.shape[1]

    weights = {"a0": (a0, wa0), "b0": (b0, wb0), "a1": (a1, wa1), "b1": (b1, wb1)}
    rows_of = [pl.ds(pl.multiple_of(place(p, tb, ta, tb_size, ta_size) * depth, depth), depth) for p in range(2 * tb_size)]

    own = [pltpu.make_async_copy(x_own, x_ref.at[me], own_sem.at[0])]
    for n, (shard, whole) in enumerate(weights.values()):
        own.append(pltpu.make_async_copy(shard, whole.at[rows_of[0], :], own_sem.at[1 + n]))
    for copy in own:
        copy.start()

    moves = {}

    def move(name, source, target, device):
        i = len(moves)
        moves[name] = pltpu.make_async_remote_copy(
            src_ref=source,
            dst_ref=target,
            send_sem=send_sem.at[i],
            recv_sem=recv_sem.at[i],
            device_id=device,
            device_id_type=pl.DeviceIdType.MESH,
        )

    for n, (shard, whole) in weights.items():
        mine, below, above, far = (whole.at[rows_of[2 * o], :] for o in range(4))
        move(n + "up", shard, mine, x_up)
        move(n + "down", shard, mine, x_down)
        move(n + "0", shard, mine, core)
        move(n + "1", below, below, core)
        move(n + "2", above, above, core)
        move(n + "3", far, far, core)
        if n[0] == "a":
            move(n + "far", below, below, x_up)
        else:
            move(n + "far", above, above, x_down)
    tall = c.shape[0] // 2
    move("cup", c, c_got.at[1], x_up)
    move("cdown", c, c_got.at[3], x_down)
    move("c0", c, c_got.at[0], core)
    move("c1", c_got.at[1], c_got.at[2], core)
    move("c2", c_got.at[3], c_got.at[4], core)
    move("c3", c_got.at[5], c_got.at[6], core)
    move("cfar0", c_got.at[1, pl.ds(0, tall)], c_got.at[5, pl.ds(0, tall)], x_up)
    move("cfar1", c_got.at[3, pl.ds(tall, tall)], c_got.at[5, pl.ds(tall, tall)], x_down)
    move("yup", x_own, x_ref.at[me], {"mp": y_up})
    move("ydown", x_own, x_ref.at[me], {"mp": y_down})
    top, low = pl.ds(0, tokens // 2), pl.ds(tokens // 2, tokens // 2)
    move("yfar0", x_ref.at[y_down, top, :], x_ref.at[y_down, top, :], {"mp": y_up})
    move("yfar1", x_ref.at[y_up, low, :], x_ref.at[y_up, low, :], {"mp": y_down})

    def stage(waits, starts):
        for n in waits.split():
            moves[n].wait_recv()
        for n in starts.split():
            moves[n].start()

    barrier = pltpu.get_barrier_semaphore()
    near = [{"mp": y_up}, {"mp": y_down}, x_up, x_down, core]
    for device in near:
        pl.semaphore_signal(barrier, inc=1, device_id=device, device_id_type=pl.DeviceIdType.MESH)
    pl.semaphore_wait(barrier, len(near))

    stage("", "a0up b0down b0up a0down yup ydown")
    stage("", "a00 b00 a10 b10 c0")
    stage("a0up b0down b0up a0down", "a0far b0far a1up b1down b1up a1down a01 a02 b01 b02")
    stage("yup ydown", "yfar0 yfar1")
    stage("a0far b0far", "a03 b03")
    stage("a1up b1down b1up a1down", "a1far b1far cup cdown a11 a12 b11 b12")
    for copy in own:
        copy.wait()
    stage("yfar0 yfar1", "")

    def norm(i, carry):
        rows = pl.ds(pl.multiple_of(i * ROWS, ROWS), ROWS)
        total = jnp.zeros((ROWS, 1), F32)
        for r in range(parts):
            xs = x_ref[r, rows, :].astype(F32)
            total += jnp.sum(xs * xs, axis=1, keepdims=True)
        inv = lax.rsqrt(total / (parts * span) + NORM_EPS)
        for r in range(parts):
            cols = slice(r * span, (r + 1) * span)
            h_ref[rows, cols] = (x_ref[r, rows, :].astype(F32) * inv * gain_ref[:, cols].astype(F32)).astype(BF16)
        return carry

    lax.fori_loop(0, tokens // ROWS, norm, 0)
    res_ref[...] = x_ref[:, pl.ds(pl.multiple_of(me * share, share), share), :]

    stage("a00 a01 a02 a03 b00 b01 b02 b03", "")

    def heads(i, carry):
        rows = pl.ds(pl.multiple_of(i * ROWS, ROWS), ROWS)
        q = dot(h_ref[rows, :], wa0[:, :width_q]).astype(BF16)
        cos_tab, sin_tab = cos_ref[rows, :], sin_ref[rows, :]
        for n in range(width_q // head_dim):
            cols = slice(n * head_dim, (n + 1) * head_dim)
            q_ref[rows, cols] = rope(q[:, cols], cos_tab, sin_tab)
        kv = dot(h_ref[rows, :], wb0[:, part_ff:]).astype(BF16)
        k_ref[rows, :] = rope(kv[:, :head_dim], cos_tab, sin_tab)
        v_ref[rows, :] = kv[:, head_dim:]
        return carry

    lax.fori_loop(0, tokens // ROWS, heads, 0)
    stage("a1far b1far", "a13 b13")

    def hidden(skip, wa, wb, base):
        tile = width_q
        count = part_ff // tile

        def body(i, carry):
            rows = pl.ds(pl.multiple_of(i // count * ROWS, ROWS), ROWS)
            at = lax.rem(i, count) * tile
            gate = dot(h_ref[rows, :], wa[:, pl.ds(pl.multiple_of(skip + at, tile), tile)]).astype(BF16).astype(F32)
            value = dot(h_ref[rows, :], wb[:, pl.ds(pl.multiple_of(at, tile), tile)]).astype(BF16).astype(F32)
            m_ref[rows, pl.ds(pl.multiple_of(base + at, tile), tile)] = (gate * (1.0 / (1.0 + jnp.exp(-gate))) * value).astype(BF16)
            return carry

        lax.fori_loop(0, tokens // ROWS * count, body, 0)

    hidden(width_q, wa0, wb0, 0)
    stage("cup cdown", "cfar0 cfar1 c1 c2")
    stage("a10 a11 a12 a13 b10 b11 b12 b13", "")
    hidden(0, wa1, wb1, part_ff)
    stage("cfar0 cfar1", "c3")
    stage("c0 c1 c2 c3", "")
    for m in moves.values():
        m.wait_send()


def first_front(x, gain, cos_tab, sin_tab, shards, width_q, width_ff, head_dim, parts, sizes, collective_id):
    tokens, span = x.shape
    embed = parts * span
    blocks = sizes[0] * sizes[1]
    vmem, far = pl.BlockSpec(memory_space=pltpu.VMEM), pl.BlockSpec(memory_space=pl.ANY)
    a0, b0, a1, b1, c = shards
    shapes = [(tokens, width_q), (tokens, head_dim), (tokens, head_dim), (tokens, width_ff), (parts, tokens // parts, span), (blocks - 1, *c.shape)]
    columns = sum(w.shape[1] for w in shards[:4])
    moves = 40
    return pl.pallas_call(
        functools.partial(first_kernel, parts, head_dim, sizes),
        in_specs=[far] + [vmem] * 3 + [far] * 5,
        out_specs=[vmem] * 5 + [far],
        out_shape=[jax.ShapeDtypeStruct(shape, BF16) for shape in shapes],
        scratch_shapes=[pltpu.VMEM((parts, tokens, span), BF16), pltpu.VMEM((tokens, embed), BF16)]
        + [pltpu.VMEM((embed, w.shape[1]), BF16) for w in shards[:4]]
        + [pltpu.SemaphoreType.DMA((5,)), pltpu.SemaphoreType.DMA((moves,)), pltpu.SemaphoreType.DMA((moves,))],
        compiler_params=pltpu.CompilerParams(vmem_limit_bytes=VMEM_LIMIT, collective_id=collective_id, has_side_effects=True),
        cost_estimate=pl.CostEstimate(flops=2 * tokens * embed * columns, bytes_accessed=2 * embed * columns, transcendentals=tokens * width_ff),
        name="first_front",
    )(x, gain, cos_tab, sin_tab, *shards)


def front_kernel(parts, head_dim, sizes, x_ref, gain_ref, cos_ref, sin_ref, a_ref, a_got, b_ref, b_got, q_ref, k_ref, v_ref, m_ref, h_ref, wa_ref, wb_ref, w_sem, send_sem, recv_sem):
    me, tb, ta = lax.axis_index("mp"), lax.axis_index("tb"), lax.axis_index("ta")
    up, down, far = lax.rem(me + 1, parts), lax.rem(me + parts - 1, parts), lax.rem(me + 2, parts)
    depth = a_ref.shape[0]
    blocks = a_got.shape[0] + 1
    half = h_ref.shape[2]
    width_q, width_ff = q_ref.shape[1], m_ref.shape[1]

    loads = []
    for p in range(blocks):
        rows = pl.ds(pl.multiple_of(place(p, tb, ta, *sizes) * depth, depth), depth)
        loads.append(pltpu.make_async_copy(a_got.at[p - 1] if p else a_ref, wa_ref.at[rows, :], w_sem.at[2 * p]))
        loads.append(pltpu.make_async_copy(b_got.at[p - 1] if p else b_ref, wb_ref.at[rows, :], w_sem.at[2 * p + 1]))
    for load in loads:
        load.start()

    barrier = pltpu.get_barrier_semaphore()
    for near in (up, down):
        pl.semaphore_signal(barrier, inc=1, device_id={"mp": near}, device_id_type=pl.DeviceIdType.MESH)

    for n in range(2):
        x = x_ref[n * half : (n + 1) * half, :]
        inv = lax.rsqrt(jnp.mean(x * x, axis=1, keepdims=True) + NORM_EPS)
        h_ref[me, n] = (x * inv * gain_ref[...].astype(F32)).astype(BF16)
    pl.semaphore_wait(barrier, 2)

    def copy(i, owner, n, to):
        return pltpu.make_async_remote_copy(
            src_ref=h_ref.at[owner, n],
            dst_ref=h_ref.at[owner, n],
            send_sem=send_sem.at[i],
            recv_sem=recv_sem.at[i],
            device_id={"mp": to},
            device_id_type=pl.DeviceIdType.MESH,
        )

    copies = [copy(0, me, 0, up), copy(1, me, 1, down), copy(2, me, 1, up), copy(3, me, 0, down), copy(4, down, 0, up), copy(5, up, 1, down)]
    for c in copies[:4]:
        c.start()
    for load in loads:
        load.wait()

    def unit(owner, n):
        rows = pl.ds(pl.multiple_of((owner * 2 + n) * half, half), half)
        q = dot(h_ref[owner, n], wa_ref[:, :width_q]).astype(BF16)
        cos_tab, sin_tab = cos_ref[rows, :], sin_ref[rows, :]
        for i in range(width_q // head_dim):
            cols = slice(i * head_dim, (i + 1) * head_dim)
            q_ref[rows, cols] = rope(q[:, cols], cos_tab, sin_tab)
        kv = dot(h_ref[owner, n], wb_ref[:, width_ff:]).astype(BF16)
        k_ref[rows, :] = rope(kv[:, :head_dim], cos_tab, sin_tab)
        v_ref[rows, :] = kv[:, head_dim:]

        def hidden(t, carry):
            at = pl.ds(pl.multiple_of(t * width_q, width_q), width_q)
            gate = dot(h_ref[owner, n], wa_ref[:, pl.ds(pl.multiple_of((t + 1) * width_q, width_q), width_q)]).astype(BF16).astype(F32)
            value = dot(h_ref[owner, n], wb_ref[:, at]).astype(BF16).astype(F32)
            m_ref[rows, at] = (gate * (1.0 / (1.0 + jnp.exp(-gate))) * value).astype(BF16)
            return carry

        lax.fori_loop(0, width_ff // width_q, hidden, 0)

    def units(first, second):
        def body(i, carry):
            unit(jnp.where(i == 0, first[0], second[0]), jnp.where(i == 0, first[1], second[1]))
            return carry

        lax.fori_loop(0, 2, body, 0)

    units((me, 0), (me, 1))
    copies[0].wait_recv()
    copies[4].start()
    copies[1].wait_recv()
    copies[5].start()
    units((down, 0), (up, 1))
    copies[2].wait_recv()
    copies[3].wait_recv()
    units((down, 1), (up, 0))
    copies[4].wait_recv()
    copies[5].wait_recv()
    units((far, 0), (far, 1))
    for c in copies:
        c.wait_send()


def front(x, gain, cos_tab, sin_tab, a, a_got, b, b_got, width_q, width_ff, head_dim, parts, sizes, collective_id):
    share, embed = x.shape
    tokens = cos_tab.shape[0]
    vmem, far = pl.BlockSpec(memory_space=pltpu.VMEM), pl.BlockSpec(memory_space=pl.ANY)
    blocks = a_got.shape[0] + 1
    shapes = [(tokens, width_q), (tokens, head_dim), (tokens, head_dim), (tokens, width_ff)]
    return pl.pallas_call(
        functools.partial(front_kernel, parts, head_dim, sizes),
        in_specs=[vmem] * 4 + [far] * 4,
        out_specs=[vmem] * 4,
        out_shape=[jax.ShapeDtypeStruct(shape, BF16) for shape in shapes],
        scratch_shapes=[
            pltpu.VMEM((parts, 2, share // 2, embed), BF16),
            pltpu.VMEM((embed, a.shape[1]), BF16),
            pltpu.VMEM((embed, b.shape[1]), BF16),
            pltpu.SemaphoreType.DMA((2 * blocks,)),
            pltpu.SemaphoreType.DMA((6,)),
            pltpu.SemaphoreType.DMA((6,)),
        ],
        compiler_params=pltpu.CompilerParams(vmem_limit_bytes=VMEM_LIMIT, collective_id=collective_id, has_side_effects=True),
        cost_estimate=pl.CostEstimate(flops=2 * tokens * embed * (a.shape[1] + b.shape[1]), bytes_accessed=2 * embed * (a.shape[1] + b.shape[1]), transcendentals=tokens * width_ff),
        name="front",
    )(x, gain, cos_tab, sin_tab, a, a_got, b, b_got)


def back_kernel(blocks, parts, last, sizes, o_ref, m_ref, res_ref, *refs):
    piece, pieces_got = refs[:2]
    if last:
        out_ref, w_ref, sent_ref, got_ref, w_sem, send_sem, recv_sem = refs[2:]
    else:
        shards = refs[2:5]
        out_ref, *gots = refs[5:9]
        w_ref, sent_ref, got_ref, w_sem, send_sem, recv_sem, x_send, x_recv = refs[9:]
    tb_size, ta_size = sizes
    me, tb, ta = lax.axis_index("mp"), lax.axis_index("tb"), lax.axis_index("ta")
    streams, hops = got_ref.shape[0], got_ref.shape[1]
    width_q = o_ref.shape[1]
    cols = w_ref.shape[2]
    high, wide = got_ref.shape[2], got_ref.shape[3]

    loads = []
    for p in range(blocks):
        at = place(p, tb, ta, tb_size, ta_size)
        loads.append(pltpu.make_async_copy(pieces_got.at[p - 1] if p else piece, w_ref.at[at], w_sem.at[p]))
    for load in loads:
        load.start()

    barrier = pltpu.get_barrier_semaphore()
    near = [{"mp": lax.rem(me + 1, parts)}, {"mp": lax.rem(me + parts - 1, parts)}]
    if not last:
        x_up, x_down = {"tb": lax.rem(tb + 1, tb_size)}, {"tb": lax.rem(tb + tb_size - 1, tb_size)}
        core = {"ta": lax.rem(ta + 1, ta_size)}
        near += [x_up, x_down, core]
    for device in near:
        pl.semaphore_signal(barrier, inc=1, device_id=device, device_id_type=pl.DeviceIdType.MESH)
    for load in loads:
        load.wait()
    pl.semaphore_wait(barrier, len(near))

    moves = {}
    if not last:
        names = "abc"
        wide_c = shards[2].shape[0] // 2

        def move(name, source, target, device):
            i = len(moves)
            moves[name] = pltpu.make_async_remote_copy(
                src_ref=source,
                dst_ref=target,
                send_sem=x_send.at[i],
                recv_sem=x_recv.at[i],
                device_id=device,
                device_id_type=pl.DeviceIdType.MESH,
            )

        for n, shard, got in zip(names, shards, gots):
            move(n + "up", shard, got.at[1], x_up)
            move(n + "down", shard, got.at[3], x_down)
            move(n + "0", shard, got.at[0], core)
            move(n + "1", got.at[1], got.at[2], core)
            move(n + "2", got.at[3], got.at[4], core)
            move(n + "3", got.at[5], got.at[6], core)
        a_got, b_got, c_got = gots
        move("afar", a_got.at[1], a_got.at[5], x_up)
        move("bfar", b_got.at[3], b_got.at[5], x_down)
        move("cfar0", c_got.at[1, pl.ds(0, wide_c)], c_got.at[5, pl.ds(0, wide_c)], x_up)
        move("cfar1", c_got.at[3, pl.ds(wide_c, wide_c)], c_got.at[5, pl.ds(wide_c, wide_c)], x_down)

    def stage(waits, starts):
        for n in waits:
            moves[n].wait_recv()
        for n in starts:
            moves[n].start()

    if not last:
        stage((), ("aup", "bdown", "bup", "adown", "a0", "b0"))

    def partial(stream, dest):
        if last:
            rows = pl.ds(pl.multiple_of(stream * high, high), high)
            first = dest * (wide // cols)
            tiles = [first + n for n in range(wide // cols)]
        else:
            rows = pl.ds(pl.multiple_of(dest * high, high), high)
            tiles = [stream]
        o, m = o_ref[rows, :], m_ref[rows, :]
        sums = [dot(o, w_ref[t, :width_q, :]) + dot(m, w_ref[t, width_q:, :]) for t in tiles]
        return sums[0] if len(sums) == 1 else jnp.concatenate(sums, axis=1)

    def hop(stream, step):
        up = stream < streams // 2
        return pltpu.make_async_remote_copy(
            src_ref=sent_ref.at[stream] if step == 0 else got_ref.at[stream, step - 1],
            dst_ref=got_ref.at[stream, step],
            send_sem=send_sem.at[stream, step],
            recv_sem=recv_sem.at[stream, step],
            device_id={"mp": lax.rem(me + jnp.where(up, 1, parts - 1), parts)},
            device_id_type=pl.DeviceIdType.MESH,
        )

    for step in range(hops + 1):

        def body(i, carry):
            if not last and step == 2:

                @pl.when(i == 2)
                def _():
                    stage(("aup", "adown", "bup", "bdown"), ("afar", "bfar", "cup", "cdown", "a1", "a2", "b1", "b2", "c0"))

            if not last and step == hops:

                @pl.when(i == 4)
                def _():
                    stage(("afar", "bfar", "cup", "cdown"), ("cfar0", "cfar1", "a3", "b3", "c1", "c2"))

            stream = lax.rem(i, 2) * (streams // 2) + i // 2
            up = stream < streams // 2
            dest = lax.rem(me + jnp.where(up, 2 * parts - 1 - step, 1 + step), parts)
            value = partial(stream, dest)
            if last:
                held = res_ref.shape[0]
                per = held // high

                def with_residual(v):
                    here = pl.ds(pl.multiple_of(lax.rem(stream, per) * high, high), high)
                    there = pl.ds(pl.multiple_of(dest * wide, wide), wide)
                    mine = jnp.where(stream // per == me, 1.0, 0.0)
                    return v + res_ref[here, there] * mine

                value = with_residual(value)
            if step > 0:
                hop(stream, step - 1).wait_recv()
                value += got_ref[stream, step - 1]
            if step == 0:
                sent_ref[stream] = value
            elif step < hops:
                got_ref[stream, step - 1] = value
            if step < hops:
                hop(stream, step).start()
            elif last:
                out_ref[pl.ds(pl.multiple_of(stream * high, high), high), :] = value
            else:
                per = res_ref.shape[2] // cols
                col = pl.ds(pl.multiple_of(lax.rem(stream, per) * cols, cols), cols)
                out_ref[:, pl.ds(pl.multiple_of(stream * cols, cols), cols)] = value + res_ref[stream // per, :, col].astype(F32)
            return carry

        lax.fori_loop(0, streams, body, 0)

    if not last:
        stage(("cfar0", "cfar1"), ("c3",))
        stage(("a0", "b0", "c0", "a1", "a2", "a3", "b1", "b2", "b3", "c1", "c2", "c3"), ())
        for m in moves.values():
            m.wait_send()

    for step in range(hops):

        def drain(stream, carry):
            hop(stream, step).wait_send()
            return carry

        lax.fori_loop(0, streams, drain, 0)


def back(o, m, res, pieces, shards, parts, sizes, last, collective_id):
    tokens, width_q = o.shape
    depth, cols = pieces[0].shape
    blocks = sizes[0] * sizes[1]
    embed = blocks * cols
    streams, hops = blocks, parts - 1
    if last:
        shape, out = (tokens // streams, embed // parts), (tokens, embed // parts)
    else:
        shape, out = (tokens // parts, cols), (tokens // parts, embed)
    vmem, far = pl.BlockSpec(memory_space=pltpu.VMEM), pl.BlockSpec(memory_space=pl.ANY)
    moves = 22
    return pl.pallas_call(
        functools.partial(back_kernel, blocks, parts, last, sizes),
        in_specs=[vmem, vmem, vmem] + [far] * (len(pieces) + len(shards)),
        out_specs=[vmem] + [far] * len(shards),
        out_shape=[jax.ShapeDtypeStruct(out, F32)] + [jax.ShapeDtypeStruct((blocks - 1, *w.shape), BF16) for w in shards],
        scratch_shapes=[
            pltpu.VMEM((blocks, depth, cols), BF16),
            pltpu.VMEM((streams, *shape), F32),
            pltpu.VMEM((streams, hops, *shape), F32),
            pltpu.SemaphoreType.DMA((blocks,)),
            pltpu.SemaphoreType.DMA((streams, hops)),
            pltpu.SemaphoreType.DMA((streams, hops)),
        ]
        + ([] if last else [pltpu.SemaphoreType.DMA((moves,))] * 2),
        compiler_params=pltpu.CompilerParams(vmem_limit_bytes=VMEM_LIMIT, collective_id=collective_id, has_side_effects=True),
        cost_estimate=pl.CostEstimate(flops=8 * tokens * depth * embed, bytes_accessed=2 * depth * embed, transcendentals=0),
        name="back",
    )(o, m, res, *pieces, *shards)


def solution(mesh):
    mp_size, tb_size, ta_size = mesh.shape["mp"], mesh.shape["tb"], mesh.shape["ta"]
    assert mp_size == 4 and tb_size == 4 and ta_size == 2
    sizes = (tb_size, ta_size)
    def device_body(x_loc, seg_ids, pos_ids, w_q, w_k, w_v, w_gate, w_up, w_out, w_down, gain):
        tokens, embed_loc = x_loc.shape
        head_dim, width_q, width_ff = w_k.shape[-1], w_q.shape[-1], w_gate.shape[-1]
        inv_freq = ROPE_BASE ** (-(jnp.arange(head_dim // 2, dtype=F32) * 2.0) / head_dim)
        angles = pos_ids.astype(F32)[:, None] * inv_freq[None, :]
        cos_tab, sin_tab = jnp.cos(angles), jnp.sin(angles)
        cos_tab = jnp.concatenate([cos_tab, cos_tab], axis=1)
        sin_tab = jnp.concatenate([-sin_tab, sin_tab], axis=1)
        start = jnp.arange(tokens, dtype=jnp.int32) - pos_ids
        low = start[::Q_TILE]
        start = start[None, :]

        half = width_ff // 2
        first = (
            jnp.concatenate([w_q[0], w_gate[0, :, :half]], axis=1),
            jnp.concatenate([w_up[0, :, :half], w_k[0], w_v[0]], axis=1),
            w_gate[0, :, half:],
            w_up[0, :, half:],
            jnp.concatenate([w_out[0], w_down[0]], axis=0),
        )
        q, k, v, m, residual, c_got = first_front(x_loc, gain[:1], cos_tab, sin_tab, first, width_q, width_ff, head_dim, mp_size, sizes, 4)
        with jax.named_scope("attn0"):
            o = attention(q, k, v, low, start)
        a = jnp.concatenate([w_q[1], w_gate[1]], axis=1)
        b = jnp.concatenate([w_up[1], w_k[1], w_v[1]], axis=1)
        c = jnp.concatenate([w_out[1], w_down[1]], axis=0)
        with jax.named_scope("back0"):
            hidden, a_got, b_got, c_got = back(o, m, residual, (first[4], c_got), (a, b, c), mp_size, sizes, False, 1)
        with jax.named_scope("front1"):
            q, k, v, m = front(hidden, gain[1:], cos_tab, sin_tab, a, a_got, b, b_got, width_q, width_ff, head_dim, mp_size, sizes, 2)
        with jax.named_scope("attn1"):
            o = attention(q, k, v, low, start)
        with jax.named_scope("back1"):
            return back(o, m, hidden, (c, c_got), (), mp_size, sizes, True, 3)[0]

    col_spec = P(None, PLANE_AXES, "mp")
    kv_spec = P(None, PLANE_AXES, None)
    row_spec = P(None, "mp", PLANE_AXES)
    return jax.shard_map(
        device_body,
        mesh=mesh,
        in_specs=(P(TOKEN_AXES, "mp"), P(TOKEN_AXES), P(TOKEN_AXES), col_spec, kv_spec, kv_spec, col_spec, col_spec, row_spec, row_spec, P(None, None)),
        out_specs=P(TOKEN_AXES, "mp"),
        check_vma=False,
    )
```

```python
import functools

import jax
import jax.numpy as jnp
import numpy as np
from jax import lax
from jax.experimental import pallas as pl
from jax.experimental.pallas import tpu as pltpu
from jax.sharding import PartitionSpec as P

ROPE_BASE = 10000.0
NORM_EPS = 1e-6
TOKEN_AXES = ("rep", "tb", "ta")
PLANE_AXES = ("tb", "ta")
F32 = jnp.float32
BF16 = jnp.bfloat16
ROWS = 512
Q_TILE = 128
K_TILE = 512
SUBS = 4
VMEM_LIMIT = 60 * 1024 * 1024


def dot(a, b):
    return jnp.dot(a, b, preferred_element_type=F32)


def rope(t, cos_tab, sin_tab):
    half = t.shape[-1] // 2
    t = t.astype(F32)
    swapped = jnp.concatenate([t[:, half:], t[:, :half]], axis=1)
    return (t * cos_tab + swapped * sin_tab).astype(BF16)


def place(p, tb, ta, tb_size, ta_size):
    return lax.rem(tb + (0, tb_size - 1, 1, 2)[p // 2], tb_size) * ta_size + lax.rem(ta + p % 2, ta_size)


def first_kernel(parts, head_dim, sizes, x_own, gain_ref, pos_ref, freq_ref, w_q, w_k, w_v, w_gate, w_up, w_out, w_down, q_out, k_out, v_out, m_out, res_ref, cos_ref, sin_ref, c_got, q_ref, k_ref, v_ref, m_ref, out_sem, x_ref, h_ref, wa0, wb0, wa1, wb1, own_sem, send_sem, recv_sem):
    tb_size, ta_size = sizes
    me, tb, ta = lax.axis_index("mp"), lax.axis_index("tb"), lax.axis_index("ta")
    y_up, y_down = lax.rem(me + 1, parts), lax.rem(me + parts - 1, parts)
    x_up, x_down = {"tb": lax.rem(tb + 1, tb_size)}, {"tb": lax.rem(tb + tb_size - 1, tb_size)}
    core = {"ta": lax.rem(ta + 1, ta_size)}
    tokens, span = x_own.shape
    depth = w_q.shape[1]
    width_q, width_ff = q_ref.shape[1], m_ref.shape[1]
    part_ff = width_ff // 2
    share = res_ref.shape[1]

    part = [pl.ds(n * part_ff, part_ff) for n in range(2)]
    arrays = {"a0": wa0, "b0": wb0, "a1": wa1, "b1": wb1}
    sources = {
        "q": (w_q.at[0], wa0, 0),
        "g0": (w_gate.at[0, :, part[0]], wa0, width_q),
        "u0": (w_up.at[0, :, part[0]], wb0, 0),
        "k": (w_k.at[0], wb0, part_ff),
        "v": (w_v.at[0], wb0, part_ff + head_dim),
        "g1": (w_gate.at[0, :, part[1]], wa1, 0),
        "u1": (w_up.at[0, :, part[1]], wb1, 0),
    }
    rows_of = [pl.ds(pl.multiple_of(place(p, tb, ta, tb_size, ta_size) * depth, depth), depth) for p in range(2 * tb_size)]

    own = [pltpu.make_async_copy(x_own, x_ref.at[me], own_sem.at[0])]
    for n, (source, whole, col) in enumerate(sources.values()):
        own.append(pltpu.make_async_copy(source, whole.at[rows_of[0], pl.ds(col, source.shape[1])], own_sem.at[1 + n]))
    for copy in own:
        copy.start()

    moves = {}

    def move(name, source, target, device):
        i = len(moves)
        moves[name] = pltpu.make_async_remote_copy(
            src_ref=source,
            dst_ref=target,
            send_sem=send_sem.at[i],
            recv_sem=recv_sem.at[i],
            device_id=device,
            device_id_type=pl.DeviceIdType.MESH,
        )

    for n, (source, whole, col) in sources.items():
        mine = whole.at[rows_of[0], pl.ds(col, source.shape[1])]
        move(n + "up", source, mine, x_up)
        move(n + "down", source, mine, x_down)
        move(n + "core", source, mine, core)
    for n, whole in arrays.items():
        mine, below, above, far = (whole.at[rows_of[2 * o], :] for o in range(4))
        move(n + "1", below, below, core)
        move(n + "2", above, above, core)
        move(n + "3", far, far, core)
        if n[0] == "a":
            move(n + "far", below, below, x_up)
        else:
            move(n + "far", above, above, x_down)
    tall = c_got.shape[1] // 2
    for n, source, row in (("o", w_out.at[0], 0), ("d0", w_down.at[0, pl.ds(0, tall - width_q)], width_q), ("d1", w_down.at[0, pl.ds(tall - width_q, tall)], tall)):
        rows = pl.ds(row, source.shape[0])
        move(n + "up", source, c_got.at[1, rows], x_up)
        move(n + "down", source, c_got.at[3, rows], x_down)
        move(n + "core", source, c_got.at[0, rows], core)
    move("c1", c_got.at[1], c_got.at[2], core)
    move("c2", c_got.at[3], c_got.at[4], core)
    move("c3", c_got.at[5], c_got.at[6], core)
    move("cfar0", c_got.at[1, pl.ds(0, tall)], c_got.at[5, pl.ds(0, tall)], x_up)
    move("cfar1", c_got.at[3, pl.ds(tall, tall)], c_got.at[5, pl.ds(tall, tall)], x_down)
    chunk = tokens // 2
    for n in range(2):
        rows, top, low = pl.ds(n * chunk, chunk), pl.ds(n * chunk, chunk // 2), pl.ds(n * chunk + chunk // 2, chunk // 2)
        move(f"yup{n}", x_own.at[rows], x_ref.at[me, rows], {"mp": y_up})
        move(f"ydown{n}", x_own.at[rows], x_ref.at[me, rows], {"mp": y_down})
        move(f"ytop{n}", x_ref.at[y_down, top], x_ref.at[y_down, top], {"mp": y_up})
        move(f"ylow{n}", x_ref.at[y_up, low], x_ref.at[y_up, low], {"mp": y_down})

    def stage(waits, starts):
        for n in waits:
            moves[n].wait_recv()
        for n in starts:
            moves[n].start()

    barrier = pltpu.get_barrier_semaphore()
    near = [{"mp": y_up}, {"mp": y_down}, x_up, x_down, core]
    for device in near:
        pl.semaphore_signal(barrier, inc=1, device_id=device, device_id_type=pl.DeviceIdType.MESH)
    pl.semaphore_wait(barrier, len(near))

    stage((), ("qup", "u0down", "g0up", "kdown", "vdown", "u0up", "qdown", "kup", "vup", "g0down", "g1up", "u1down", "yup0", "ydown0", "qcore", "g0core", "u0core", "kcore", "vcore"))

    def rotary(i, carry):
        rows = pl.ds(pl.multiple_of(i * ROWS, ROWS), ROWS)
        angles = jnp.broadcast_to(pos_ref[:, rows].astype(F32), (head_dim, ROWS)).T * freq_ref[:1, :]
        cos_ref[rows, :] = jnp.cos(angles)
        sin_ref[rows, :] = jnp.sin(angles) * freq_ref[1:, :]
        return carry

    lax.fori_loop(0, tokens // ROWS, rotary, 0)
    stage(("yup0", "ydown0"), ("ytop0", "ylow0", "yup1", "ydown1"))
    stage(("qup", "g0up", "u0up", "kup", "vup", "qdown", "g0down", "u0down", "kdown", "vdown"), ("a0far", "b0far", "u1up", "g1down", "oup", "d1down", "a01", "a02", "b01", "b02", "g1core", "u1core"))
    for copy in own:
        copy.wait()

    def norm(i, carry):
        rows = pl.ds(pl.multiple_of(i * ROWS, ROWS), ROWS)
        total = jnp.zeros((ROWS, 1), F32)
        for r in range(parts):
            xs = x_ref[r, rows, :].astype(F32)
            total += jnp.sum(xs * xs, axis=1, keepdims=True)
        inv = lax.rsqrt(total / (parts * span) + NORM_EPS)
        for r in range(parts):
            cols = slice(r * span, (r + 1) * span)
            h_ref[rows, cols] = (x_ref[r, rows, :].astype(F32) * inv * gain_ref[:1, cols].astype(F32)).astype(BF16)
        return carry

    blocks = chunk // ROWS
    stage(("ytop0", "ylow0"), ())
    lax.fori_loop(0, blocks, norm, 0)
    stage(("a0far", "b0far"), ("a03", "b03"))
    stage(("qcore", "g0core", "u0core", "kcore", "vcore", "a01", "a02", "a03", "b01", "b02", "b03"), ())

    def heads(i, carry):
        rows = pl.ds(pl.multiple_of(i * ROWS, ROWS), ROWS)
        q = dot(h_ref[rows, :], wa0[:, :width_q]).astype(BF16)
        cos_tab, sin_tab = cos_ref[rows, :], sin_ref[rows, :]
        for n in range(width_q // head_dim):
            cols = slice(n * head_dim, (n + 1) * head_dim)
            q_ref[rows, cols] = rope(q[:, cols], cos_tab, sin_tab)
        kv = dot(h_ref[rows, :], wb0[:, part_ff:]).astype(BF16)
        k_ref[rows, :] = rope(kv[:, :head_dim], cos_tab, sin_tab)
        v_ref[rows, :] = kv[:, head_dim:]
        return carry

    def hidden(n, skip, wa, wb, base):
        tile = width_q
        count = part_ff // tile

        def body(i, carry):
            rows = pl.ds(pl.multiple_of(n * chunk + i // count * ROWS, ROWS), ROWS)
            at = lax.rem(i, count) * tile
            gate = dot(h_ref[rows, :], wa[:, pl.ds(pl.multiple_of(skip + at, tile), tile)]).astype(BF16).astype(F32)
            value = dot(h_ref[rows, :], wb[:, pl.ds(pl.multiple_of(at, tile), tile)]).astype(BF16).astype(F32)
            m_ref[rows, pl.ds(pl.multiple_of(base + at, tile), tile)] = (gate * (1.0 / (1.0 + jnp.exp(-gate))) * value).astype(BF16)
            return carry

        lax.fori_loop(0, blocks * count, body, 0)
        leave(m_ref, m_out, pl.ds(n * chunk, chunk), pl.ds(base, part_ff))

    leaving = []

    def leave(source, target, *index):
        copy = pltpu.make_async_copy(source.at[index], target.at[index], out_sem.at[len(leaving)])
        copy.start()
        leaving.append(copy)

    def heads_of(n):
        lax.fori_loop(n * blocks, (n + 1) * blocks, heads, 0)
        for source, target in ((q_ref, q_out), (k_ref, k_out), (v_ref, v_out)):
            leave(source, target, pl.ds(n * chunk, chunk))

    heads_of(0)
    stage(("yup1", "ydown1"), ("ytop1", "ylow1"))
    hidden(0, width_q, wa0, wb0, 0)
    stage(("g1up", "g1down", "u1up", "u1down"), ("a1far", "b1far", "d0up", "odown", "d1up", "d0down", "a11", "a12", "b11", "b12", "ocore", "d0core", "d1core"))
    stage(("ytop1", "ylow1"), ())
    lax.fori_loop(blocks, 2 * blocks, norm, 0)
    res_ref[...] = x_ref[:, pl.ds(pl.multiple_of(me * share, share), share), :]
    heads_of(1)
    stage(("a1far", "b1far"), ("a13", "b13"))
    hidden(1, width_q, wa0, wb0, 0)
    stage(("oup", "d0up", "d1down"), ("cfar0", "cfar1"))
    stage(("g1core", "u1core", "a11", "a12", "a13", "b11", "b12", "b13"), ())
    hidden(0, 0, wa1, wb1, part_ff)
    stage(("d1up", "odown", "d0down"), ("c1", "c2"))
    hidden(1, 0, wa1, wb1, part_ff)
    stage(("cfar0", "cfar1"), ("c3",))
    stage(("ocore", "d0core", "d1core", "c1", "c2", "c3"), ())
    for copy in leaving:
        copy.wait()
    for m in moves.values():
        m.wait_send()


def first_front(x, gain, pos, freq, shards, width_q, width_ff, head_dim, parts, sizes, collective_id):
    tokens, span = x.shape
    embed = parts * span
    blocks = sizes[0] * sizes[1]
    vmem, far = pl.BlockSpec(memory_space=pltpu.VMEM), pl.BlockSpec(memory_space=pl.ANY)
    w_out, w_down = shards[5:]
    deep = w_out.shape[1] + w_down.shape[1]
    shapes = [(tokens, width_q), (tokens, head_dim), (tokens, head_dim), (tokens, width_ff), (parts, tokens // parts, span), (tokens, head_dim), (tokens, head_dim), (blocks - 1, deep, w_out.shape[2])]
    part_ff = width_ff // 2
    widths = (width_q + part_ff, part_ff + 2 * head_dim, part_ff, part_ff)
    columns = sum(widths)
    moves = 59
    return pl.pallas_call(
        functools.partial(first_kernel, parts, head_dim, sizes),
        in_specs=[far] + [vmem] * 3 + [far] * 7,
        out_specs=[far] * 4 + [vmem] * 3 + [far],
        out_shape=[jax.ShapeDtypeStruct(shape, F32 if i in (5, 6) else BF16) for i, shape in enumerate(shapes)],
        scratch_shapes=[pltpu.VMEM(shape, BF16) for shape in shapes[:4]]
        + [pltpu.SemaphoreType.DMA((10,)), pltpu.VMEM((parts, tokens, span), BF16), pltpu.VMEM((tokens, embed), BF16)]
        + [pltpu.VMEM((embed, w), BF16) for w in widths]
        + [pltpu.SemaphoreType.DMA((8,)), pltpu.SemaphoreType.DMA((moves,)), pltpu.SemaphoreType.DMA((moves,))],
        compiler_params=pltpu.CompilerParams(vmem_limit_bytes=VMEM_LIMIT, collective_id=collective_id, has_side_effects=True),
        cost_estimate=pl.CostEstimate(flops=2 * tokens * embed * columns, bytes_accessed=2 * embed * columns, transcendentals=tokens * width_ff),
        name="first_front",
    )(x, gain, pos, freq, *shards)


def front_kernel(parts, head_dim, sizes, x_ref, gain_ref, cos_ref, sin_ref, w_q, w_k, w_v, w_gate, w_up, a_got, b_got, q_out, k_out, v_out, m_out, q_ref, k_ref, v_ref, m_ref, out_sem, h_ref, wa_ref, wb_ref, w_sem, send_sem, recv_sem):
    me, tb, ta = lax.axis_index("mp"), lax.axis_index("tb"), lax.axis_index("ta")
    up, down, far = lax.rem(me + 1, parts), lax.rem(me + parts - 1, parts), lax.rem(me + 2, parts)
    depth = w_q.shape[1]
    blocks = a_got.shape[0] + 1
    half = h_ref.shape[2]
    width_q, width_ff = q_ref.shape[1], m_ref.shape[1]

    loads = []

    def load(source, target):
        loads.append(pltpu.make_async_copy(source, target, w_sem.at[len(loads)]))

    for p in range(blocks):
        rows = pl.ds(pl.multiple_of(place(p, tb, ta, *sizes) * depth, depth), depth)
        if p:
            load(a_got.at[p - 1], wa_ref.at[rows, :])
            load(b_got.at[p - 1], wb_ref.at[rows, :])
        else:
            load(w_q.at[1], wa_ref.at[rows, pl.ds(0, width_q)])
            load(w_gate.at[1], wa_ref.at[rows, pl.ds(width_q, width_ff)])
            load(w_up.at[1], wb_ref.at[rows, pl.ds(0, width_ff)])
            load(w_k.at[1], wb_ref.at[rows, pl.ds(width_ff, head_dim)])
            load(w_v.at[1], wb_ref.at[rows, pl.ds(width_ff + head_dim, head_dim)])
    for one in loads:
        one.start()

    barrier = pltpu.get_barrier_semaphore()
    for near in (up, down):
        pl.semaphore_signal(barrier, inc=1, device_id={"mp": near}, device_id_type=pl.DeviceIdType.MESH)

    def norm(n):
        x = x_ref[n * half : (n + 1) * half, :]
        inv = lax.rsqrt(jnp.mean(x * x, axis=1, keepdims=True) + NORM_EPS)
        h_ref[me, n] = (x * inv * gain_ref[1:, :].astype(F32)).astype(BF16)

    subs = h_ref.shape[1]

    def copy(i, owner, n, to):
        return pltpu.make_async_remote_copy(
            src_ref=h_ref.at[owner, n],
            dst_ref=h_ref.at[owner, n],
            send_sem=send_sem.at[i],
            recv_sem=recv_sem.at[i],
            device_id={"mp": to},
            device_id_type=pl.DeviceIdType.MESH,
        )

    rising = [copy(n, me, n, up) for n in range(subs)]
    falling = [copy(subs + n, me, subs - 1 - n, down) for n in range(subs)]
    on_up = [copy(2 * subs + n, down, n, up) for n in range(subs // 2)]
    on_down = [copy(2 * subs + subs // 2 + n, up, subs - 1 - n, down) for n in range(subs // 2)]
    norm(0)
    norm(subs - 1)
    pl.semaphore_wait(barrier, 2)
    rising[0].start()
    falling[0].start()
    for n in range(1, subs - 1):
        norm(n)
    for n in range(1, subs):
        rising[n].start()
        falling[n].start()
    for one in loads:
        one.wait()

    def leave(piece):
        rows = pl.ds(pl.multiple_of(piece * half, half), half)
        pairs = ((q_ref, q_out), (k_ref, k_out), (v_ref, v_out), (m_ref, m_out))
        return [pltpu.make_async_copy(source.at[rows, :], target.at[rows, :], out_sem.at[piece, n]) for n, (source, target) in enumerate(pairs)]

    def unit(owner, n):
        rows = pl.ds(pl.multiple_of((owner * subs + n) * half, half), half)
        q = dot(h_ref[owner, n], wa_ref[:, :width_q]).astype(BF16)
        cos_tab, sin_tab = cos_ref[rows, :], sin_ref[rows, :]
        for i in range(width_q // head_dim):
            cols = slice(i * head_dim, (i + 1) * head_dim)
            q_ref[rows, cols] = rope(q[:, cols], cos_tab, sin_tab)
        kv = dot(h_ref[owner, n], wb_ref[:, width_ff:]).astype(BF16)
        k_ref[rows, :] = rope(kv[:, :head_dim], cos_tab, sin_tab)
        v_ref[rows, :] = kv[:, head_dim:]

        def hidden(t, carry):
            at = pl.ds(pl.multiple_of(t * width_q, width_q), width_q)
            gate = dot(h_ref[owner, n], wa_ref[:, pl.ds(pl.multiple_of((t + 1) * width_q, width_q), width_q)]).astype(BF16).astype(F32)
            value = dot(h_ref[owner, n], wb_ref[:, at]).astype(BF16).astype(F32)
            m_ref[rows, at] = (gate * (1.0 / (1.0 + jnp.exp(-gate))) * value).astype(BF16)
            return carry

        lax.fori_loop(0, width_ff // width_q, hidden, 0)
        for copy in leave(owner * subs + n):
            copy.start()

    def units(first, second):
        def body(i, carry):
            unit(jnp.where(i == 0, first[0], second[0]), jnp.where(i == 0, first[1], second[1]))
            return carry

        lax.fori_loop(0, 2, body, 0)

    def mine(n, carry):
        unit(me, n)
        return carry

    lax.fori_loop(0, subs, mine, 0)
    for n in range(subs):
        rising[n].wait_recv()
        falling[n].wait_recv()
        if n < subs // 2:
            on_up[n].start()
            on_down[n].start()
        units((down, n), (up, subs - 1 - n))
    for n in range(subs // 2):
        on_up[n].wait_recv()
        on_down[n].wait_recv()
        units((far, n), (far, subs - 1 - n))
    for c in rising + falling + on_up + on_down:
        c.wait_send()

    def left(piece, carry):
        for copy in leave(piece):
            copy.wait()
        return carry

    lax.fori_loop(0, parts * subs, left, 0)


def front(x, gain, cos_tab, sin_tab, weights, a_got, b_got, width_q, width_ff, head_dim, parts, sizes, collective_id):
    share, embed = x.shape
    tokens = cos_tab.shape[0]
    vmem, far = pl.BlockSpec(memory_space=pltpu.VMEM), pl.BlockSpec(memory_space=pl.ANY)
    blocks = a_got.shape[0] + 1
    shapes = [(tokens, width_q), (tokens, head_dim), (tokens, head_dim), (tokens, width_ff)]
    return pl.pallas_call(
        functools.partial(front_kernel, parts, head_dim, sizes),
        in_specs=[vmem] * 4 + [far] * 7,
        out_specs=[far] * 4,
        out_shape=[jax.ShapeDtypeStruct(shape, BF16) for shape in shapes],
        scratch_shapes=[pltpu.VMEM(shape, BF16) for shape in shapes]
        + [
            pltpu.SemaphoreType.DMA((parts * SUBS, 4)),
            pltpu.VMEM((parts, SUBS, share // SUBS, embed), BF16),
            pltpu.VMEM((embed, a_got.shape[2]), BF16),
            pltpu.VMEM((embed, b_got.shape[2]), BF16),
            pltpu.SemaphoreType.DMA((2 * blocks + 3,)),
            pltpu.SemaphoreType.DMA((3 * SUBS,)),
            pltpu.SemaphoreType.DMA((3 * SUBS,)),
        ],
        compiler_params=pltpu.CompilerParams(vmem_limit_bytes=VMEM_LIMIT, collective_id=collective_id, has_side_effects=True),
        cost_estimate=pl.CostEstimate(flops=2 * tokens * embed * (a_got.shape[2] + b_got.shape[2]), bytes_accessed=2 * embed * (a_got.shape[2] + b_got.shape[2]), transcendentals=tokens * width_ff),
        name="front",
    )(x, gain, cos_tab, sin_tab, *weights, a_got, b_got)


def attend(head_dim, tile, pos_ref, q_ref, k_ref, v_ref, o_ref, s_ref, acc_ref):
    rows = Q_TILE
    heads = q_ref.shape[1] // head_dim
    scale = head_dim**-0.5
    first = tile * rows
    at = pl.ds(pl.multiple_of(first, rows), rows)
    q = jnp.concatenate([q_ref[at, i * head_dim : (i + 1) * head_dim] for i in range(heads)], axis=0)
    own = first + lax.broadcasted_iota(jnp.int32, (1, rows), 1)
    start = own - pos_ref[:, at]
    count = (first + rows + K_TILE - 1) // K_TILE

    def score(t, peak):
        keys = pl.ds(pl.multiple_of(t * K_TILE, K_TILE), K_TILE)
        s = lax.dot_general(k_ref[keys, :], q, (((1,), (1,)), ((), ())), preferred_element_type=F32) * scale
        key = t * K_TILE + lax.broadcasted_iota(jnp.int32, (K_TILE, rows), 0)
        allowed = (key >= start) & (key <= own)
        s = jnp.concatenate([jnp.where(allowed, s[:, i * rows : (i + 1) * rows], -1e30) for i in range(heads)], axis=1)
        s_ref[t] = s
        return jnp.maximum(peak, jnp.max(s, axis=0, keepdims=True))

    peak = lax.fori_loop(0, count, score, jnp.full((1, heads * rows), -1e30, F32))

    def expo(t, total):
        e = jnp.exp(s_ref[t] - peak)
        s_ref[t] = e
        return total + jnp.sum(e, axis=0, keepdims=True)

    inv = 1.0 / lax.fori_loop(0, count, expo, jnp.zeros((1, heads * rows), F32))
    acc_ref[...] = jnp.zeros_like(acc_ref)

    def value(t, carry):
        keys = pl.ds(pl.multiple_of(t * K_TILE, K_TILE), K_TILE)
        p = (s_ref[t] * inv).astype(BF16)
        acc_ref[...] += lax.dot_general(v_ref[keys, :], p, (((0,), (0,)), ((), ())), preferred_element_type=F32)
        return carry

    lax.fori_loop(0, count, value, 0)
    for i in range(heads):
        o_ref[at, i * head_dim : (i + 1) * head_dim] = acc_ref[:, i * rows : (i + 1) * rows].T.astype(BF16)


def back_kernel(blocks, parts, last, sizes, pos_ref, q_ref, k_ref, v_ref, m_far, res_ref, *refs):
    own_out, own_down, pieces_got = refs[:3]
    if last:
        out_far, out_ref, out_sem, o_ref, m_ref, s_ref, acc_ref, w_ref, sent_ref, got_ref, own_sem, row_sem, w_sem, send_sem, recv_sem = refs[3:]
    else:
        w_q, w_k, w_v, w_gate, w_up = refs[3:8]
        out_far, *gots = refs[8:12]
        out_ref, out_sem, o_ref, m_ref, s_ref, acc_ref, w_ref, sent_ref, got_ref, own_sem, row_sem, w_sem, send_sem, recv_sem, x_send, x_recv = refs[12:]
    layer = 1 if last else 0
    tb_size, ta_size = sizes
    me, tb, ta = lax.axis_index("mp"), lax.axis_index("tb"), lax.axis_index("ta")
    streams, hops = got_ref.shape[0], got_ref.shape[1]
    width_q = q_ref.shape[1]
    cols = w_ref.shape[2]
    high, wide = got_ref.shape[2], got_ref.shape[3]

    tiles = o_ref.shape[0] // Q_TILE
    per_dest = blocks // parts

    def load_rows(tile):
        rows = pl.ds(pl.multiple_of(tile * Q_TILE, Q_TILE), Q_TILE)
        return pltpu.make_async_copy(m_far.at[rows, :], m_ref.at[rows, :], row_sem.at[tile])

    def fill_rows(tile):
        attend(k_ref.shape[1], tile, pos_ref, q_ref, k_ref, v_ref, o_ref, s_ref, acc_ref)
        load_rows(tile).wait()

    own_at = place(0, tb, ta, tb_size, ta_size)
    own = (
        pltpu.make_async_copy(own_out.at[layer], w_ref.at[own_at, pl.ds(0, width_q)], own_sem.at[0]),
        pltpu.make_async_copy(own_down.at[layer], w_ref.at[own_at, pl.ds(width_q, own_down.shape[1])], own_sem.at[1]),
    )

    def wait_tile(tile):
        @pl.when(tile != own_at)
        def _():
            pltpu.make_async_copy(pieces_got.at[0], w_ref.at[tile], w_sem.at[tile]).wait()

    if last:
        row_order = list(range(tiles))
    else:
        quarters = [lax.rem(me + parts - 1, parts), lax.rem(me + 1, parts), lax.rem(me + 2, parts), me]
        row_order = [d * (tiles // parts) + n for d in quarters for n in range(tiles // parts)]
    for tile in row_order[:2]:
        load_rows(tile).start()
    for load in own:
        load.start()
    for p in range(1, blocks):
        at = place(p, tb, ta, tb_size, ta_size)
        pltpu.make_async_copy(pieces_got.at[p - 1], w_ref.at[at], w_sem.at[at]).start()
    for tile in row_order[2:]:
        load_rows(tile).start()

    barrier = pltpu.get_barrier_semaphore()
    near = [{"mp": lax.rem(me + 1, parts)}, {"mp": lax.rem(me + parts - 1, parts)}]
    if not last:
        x_up, x_down = {"tb": lax.rem(tb + 1, tb_size)}, {"tb": lax.rem(tb + tb_size - 1, tb_size)}
        core = {"ta": lax.rem(ta + 1, ta_size)}
        near += [x_up, x_down, core]
    for device in near:
        pl.semaphore_signal(barrier, inc=1, device_id=device, device_id_type=pl.DeviceIdType.MESH)
    for load in own:
        load.wait()
    pl.semaphore_wait(barrier, len(near))

    moves = {}
    if not last:
        a_got, b_got, c_got = gots
        wide_c = c_got.shape[1] // 2
        width_ff, head_dim = w_up.shape[2], w_k.shape[2]

        def move(name, source, target, device):
            i = len(moves)
            moves[name] = pltpu.make_async_remote_copy(
                src_ref=source,
                dst_ref=target,
                send_sem=x_send.at[i],
                recv_sem=x_recv.at[i],
                device_id=device,
                device_id_type=pl.DeviceIdType.MESH,
            )

        sources = {
            "q": (w_q, a_got, slice(None), pl.ds(0, width_q)),
            "g": (w_gate, a_got, slice(None), pl.ds(width_q, width_ff)),
            "u": (w_up, b_got, slice(None), pl.ds(0, width_ff)),
            "k": (w_k, b_got, slice(None), pl.ds(width_ff, head_dim)),
            "v": (w_v, b_got, slice(None), pl.ds(width_ff + head_dim, head_dim)),
            "o": (own_out, c_got, pl.ds(0, width_q), slice(None)),
            "d": (own_down, c_got, pl.ds(width_q, own_down.shape[1]), slice(None)),
        }
        for n, (source, got, high_at, wide_at) in sources.items():
            move(n + "up", source.at[1], got.at[1, high_at, wide_at], x_up)
            move(n + "down", source.at[1], got.at[3, high_at, wide_at], x_down)
            move(n + "core", source.at[1], got.at[0, high_at, wide_at], core)
        for n, got in zip("abc", gots):
            move(n + "1", got.at[1], got.at[2], core)
            move(n + "2", got.at[3], got.at[4], core)
            move(n + "3", got.at[5], got.at[6], core)
        move("afar", a_got.at[1], a_got.at[5], x_up)
        move("bfar", b_got.at[3], b_got.at[5], x_down)
        move("cfar0", c_got.at[1, pl.ds(0, wide_c)], c_got.at[5, pl.ds(0, wide_c)], x_up)
        move("cfar1", c_got.at[3, pl.ds(wide_c, wide_c)], c_got.at[5, pl.ds(wide_c, wide_c)], x_down)

    def stage(waits, starts):
        for n in waits:
            moves[n].wait_recv()
        for n in starts:
            moves[n].start()

    if not last:
        stage((), ("qup", "gup", "udown", "kdown", "vdown", "uup", "kup", "vup", "qdown", "gdown", "qcore", "gcore", "ucore", "kcore", "vcore"))

    half = streams // 2

    def block_of(stream):
        return 2 * lax.rem(stream, half) + stream // half

    def partial(stream, dest):
        if last:
            at = block_of(stream) * high
            columns = [dest * per_dest + n for n in range(per_dest)]
        else:
            at = dest * (half * high) + lax.rem(stream, half) * high
            columns = [stream // half * (wide // cols) + n for n in range(wide // cols)]
        rows = pl.ds(pl.multiple_of(at, high), high)
        o, m = o_ref[rows, :], m_ref[rows, :]
        return jnp.concatenate([dot(o, w_ref[t, :width_q, :]) + dot(m, w_ref[t, width_q:, :]) for t in columns], axis=1)

    def leave(stream):
        if last:
            at = (pl.ds(pl.multiple_of(block_of(stream) * high, high), high), slice(None))
        else:
            at = (pl.ds(pl.multiple_of(lax.rem(stream, half) * high, high), high), pl.ds(pl.multiple_of(stream // half * wide, wide), wide))
        return pltpu.make_async_copy(out_ref.at[at], out_far.at[at], out_sem.at[stream])

    def hop(stream, step):
        up = stream < streams // 2
        return pltpu.make_async_remote_copy(
            src_ref=sent_ref.at[stream] if step == 0 else got_ref.at[stream, step - 1],
            dst_ref=got_ref.at[stream, step],
            send_sem=send_sem.at[stream, step],
            recv_sem=recv_sem.at[stream, step],
            device_id={"mp": lax.rem(me + jnp.where(up, 1, parts - 1), parts)},
            device_id_type=pl.DeviceIdType.MESH,
        )

    def advance(step, pair):
        def body(side, carry):
            i = 2 * pair + side
            if not last and step == 2:

                @pl.when(i == 2)
                def _():
                    stage(("qup", "gup", "uup", "kup", "vup", "qdown", "gdown", "udown", "kdown", "vdown"), ("afar", "bfar", "oup", "dup", "odown", "ddown", "a1", "a2", "b1", "b2", "ocore", "dcore"))

            if not last and step == hops:

                @pl.when(i == 4)
                def _():
                    stage(("afar", "bfar", "oup", "dup", "odown", "ddown"), ("cfar0", "cfar1", "a3", "b3", "c1", "c2"))

            stream = lax.rem(i, 2) * (streams // 2) + i // 2
            up = stream < streams // 2
            dest = lax.rem(me + jnp.where(up, 2 * parts - 1 - step, 1 + step), parts)
            if last:
                if step == 0:
                    for n in range(high // Q_TILE):
                        fill_rows(block_of(stream) * (high // Q_TILE) + n)
                if step in (0, 1, hops):

                    @pl.when(i < (2 if step == 0 else 1))
                    def _():
                        for n in range(per_dest):
                            wait_tile(dest * per_dest + n)

            else:
                mine = dest * half + lax.rem(stream, half)
                if step == 0:
                    fill_rows(mine)

                    @pl.when(i < 2)
                    def _():
                        for n in range(wide // cols):
                            wait_tile(stream // half * (wide // cols) + n)

                elif step in (1, hops):

                    @pl.when(lax.rem(i, 2) == 0)
                    def _():
                        fill_rows(mine)

            value = partial(stream, dest)
            if last:
                held = res_ref.shape[0]
                per = held // high

                def with_residual(v):
                    here = pl.ds(pl.multiple_of(lax.rem(block_of(stream), per) * high, high), high)
                    there = pl.ds(pl.multiple_of(dest * wide, wide), wide)
                    mine = jnp.where(block_of(stream) // per == me, 1.0, 0.0)
                    return v + res_ref[here, there] * mine

                value = with_residual(value)
            if step > 0:
                hop(stream, step - 1).wait_recv()
                value += got_ref[stream, step - 1]
            if step == 0:
                sent_ref[stream] = value
            elif step < hops:
                got_ref[stream, step - 1] = value
            if step < hops:
                hop(stream, step).start()
            elif last:
                out_ref[pl.ds(pl.multiple_of(block_of(stream) * high, high), high), :] = value
            else:
                rows = pl.ds(pl.multiple_of(lax.rem(stream, half) * high, high), high)
                per = wide // res_ref.shape[2]
                side = stream // half
                kept = jnp.concatenate([res_ref[side * per + n, rows, :] for n in range(per)], axis=1)
                out_ref[rows, pl.ds(pl.multiple_of(side * wide, wide), wide)] = value + kept.astype(F32)
            if step == hops:
                leave(stream).start()
            return carry

        lax.fori_loop(0, 2, body, 0)

    def wave(w, carry):
        for step in reversed(range(hops + 1)):
            pair = w - 2 * step

            @pl.when((pair >= 0) & (pair < half))
            def _():
                advance(step, pair)

        return carry

    lax.fori_loop(0, 2 * hops + half, wave, 0)

    if not last:
        stage(("cfar0", "cfar1"), ("c3",))
        stage(("qcore", "gcore", "ucore", "kcore", "vcore", "ocore", "dcore", "a1", "a2", "a3", "b1", "b2", "b3", "c1", "c2", "c3"), ())
        for m in moves.values():
            m.wait_send()

    def gone(stream, carry):
        leave(stream).wait()
        return carry

    lax.fori_loop(0, streams, gone, 0)

    for step in range(hops):

        def drain(stream, carry):
            hop(stream, step).wait_send()
            return carry

        lax.fori_loop(0, streams, drain, 0)


def back(pos, q, k, v, m, res, w_out, w_down, c_got, weights, parts, sizes, last, collective_id):
    tokens, width_q = q.shape
    depth, cols = c_got.shape[1:]
    blocks = sizes[0] * sizes[1]
    embed = blocks * cols
    streams, hops = blocks, parts - 1
    if last:
        shape, out = (tokens // streams, embed // parts), (tokens, embed // parts)
    else:
        shape, out = (tokens // (parts * (streams // 2)), embed // 2), (tokens // parts, embed)
    vmem, far = pl.BlockSpec(memory_space=pltpu.VMEM), pl.BlockSpec(memory_space=pl.ANY)
    moves = 34
    stacked = width_q // k.shape[1] * Q_TILE
    nexts = []
    if not last:
        w_q, w_k, w_v, w_gate, w_up = weights
        rows = w_q.shape[1]
        nexts = [(rows, w_q.shape[2] + w_gate.shape[2]), (rows, w_up.shape[2] + w_k.shape[2] + w_v.shape[2]), (depth, cols)]
    return pl.pallas_call(
        functools.partial(back_kernel, blocks, parts, last, sizes),
        in_specs=[vmem] * 4 + [far, vmem] + [far] * (3 + len(weights)),
        out_specs=[far] * (1 + len(nexts)),
        out_shape=[jax.ShapeDtypeStruct(out, F32)] + [jax.ShapeDtypeStruct((blocks - 1, *shape), BF16) for shape in nexts],
        scratch_shapes=[
            pltpu.VMEM(out, F32),
            pltpu.SemaphoreType.DMA((streams,)),
            pltpu.VMEM(q.shape, BF16),
            pltpu.VMEM(m.shape, BF16),
            pltpu.VMEM((tokens // K_TILE, K_TILE, stacked), F32),
            pltpu.VMEM((k.shape[1], stacked), F32),
            pltpu.VMEM((blocks, depth, cols), BF16),
            pltpu.VMEM((streams, *shape), F32),
            pltpu.VMEM((streams, hops, *shape), F32),
            pltpu.SemaphoreType.DMA((2,)),
            pltpu.SemaphoreType.DMA((tokens // Q_TILE,)),
            pltpu.SemaphoreType.DMA((blocks,)),
            pltpu.SemaphoreType.DMA((streams, hops)),
            pltpu.SemaphoreType.DMA((streams, hops)),
        ]
        + ([] if last else [pltpu.SemaphoreType.DMA((moves,))] * 2),
        compiler_params=pltpu.CompilerParams(vmem_limit_bytes=VMEM_LIMIT, collective_id=collective_id, has_side_effects=True),
        cost_estimate=pl.CostEstimate(flops=8 * tokens * depth * embed, bytes_accessed=2 * depth * embed, transcendentals=0),
        name="back",
    )(pos, q, k, v, m, res, w_out, w_down, c_got, *weights)


def solution(mesh):
    mp_size, tb_size, ta_size = mesh.shape["mp"], mesh.shape["tb"], mesh.shape["ta"]
    assert mp_size == 4 and tb_size == 4 and ta_size == 2
    sizes = (tb_size, ta_size)
    def device_body(x_loc, seg_ids, pos_ids, w_q, w_k, w_v, w_gate, w_up, w_out, w_down, gain):
        tokens, embed_loc = x_loc.shape
        head_dim, width_q, width_ff = w_k.shape[-1], w_q.shape[-1], w_gate.shape[-1]
        half = head_dim // 2
        freq = np.float32(ROPE_BASE) ** (-(np.arange(half, dtype=np.float32) * np.float32(2.0)) / np.float32(head_dim))
        freq = np.stack([np.concatenate([freq, freq]), np.repeat(np.float32([-1.0, 1.0]), half)]).astype(np.float32)
        pos = pos_ids[None, :]

        weights = (w_q, w_k, w_v, w_gate, w_up)
        q, k, v, m, residual, cos_tab, sin_tab, c_got = first_front(
            x_loc, gain, pos, jnp.asarray(freq), (*weights, w_out, w_down), width_q, width_ff, head_dim, mp_size, sizes, 4
        )
        with jax.named_scope("back0"):
            hidden, a_got, b_got, c_got = back(pos, q, k, v, m, residual, w_out, w_down, c_got, weights, mp_size, sizes, False, 1)
        with jax.named_scope("front1"):
            q, k, v, m = front(hidden, gain, cos_tab, sin_tab, weights, a_got, b_got, width_q, width_ff, head_dim, mp_size, sizes, 2)
        with jax.named_scope("back1"):
            return back(pos, q, k, v, m, hidden, w_out, w_down, c_got, (), mp_size, sizes, True, 3)[0]

    col_spec = P(None, PLANE_AXES, "mp")
    kv_spec = P(None, PLANE_AXES, None)
    row_spec = P(None, "mp", PLANE_AXES)
    return jax.shard_map(
        device_body,
        mesh=mesh,
        in_specs=(P(TOKEN_AXES, "mp"), P(TOKEN_AXES), P(TOKEN_AXES), col_spec, kv_spec, kv_spec, col_spec, col_spec, row_spec, row_spec, P(None, None)),
        out_specs=P(TOKEN_AXES, "mp"),
        check_vma=False,
    )
```
